32 devices in a mesh: gx: 4 (over x, core), gy: 2 (over y), gz: 4 (over z).
Axes of the slice: x: 2, y: 2, z: 4, core: 2. Of those that a mesh axis runs over, the one named last changes fastest.
Arguments:
- query: bfloat16 [8, 32, 128], replicated, may hold values from -12 to 12
- k_cache: bfloat16 [8, 8192, 8, 128], P(None, ('gx', 'gy', 'gz')), may hold values from -6 to 6
- v_cache: bfloat16 [8, 8192, 8, 128], P(None, ('gx', 'gy', 'gz')), may hold values from -6 to 6
- head_gain: float32 [32, 128], replicated, may hold values from 0.5 to 1.5
Outputs:
- attended: float32 [8, 32, 128], replicated
- log_norm: float32 [8, 32], replicated
- max_logit: float32 [8, 32], replicated
The draws below stay inside these ranges and needn't reach their ends.
All inputs are finite; a program needn't handle non-finite values.
Results may differ from the reference program's by a relative error of at most 0.0003.
Values sent between devices are 32-bit elements.
A program may use at most 64 MiB of HBM per device.

```python
import jax
import jax.numpy as jnp
from jax import lax

HEADS = 32
KV_HEADS = 8
HEAD_DIM = 128
BATCH = 8
SEQ = 8192
GROUP = 4


def block_levels(own_key, shape, pieces, low, largest):
    def one(dim, shards_of):
        draws = jax.random.uniform(jax.random.fold_in(jax.random.fold_in(own_key, 6), dim), (shards_of,), jnp.float32, low / len(pieces), largest / len(pieces))
        return jnp.repeat(jnp.exp(draws), shape[dim] // shards_of).reshape((-1,) + (1,) * (len(shape) - dim - 1))

    loudness = one(*pieces[0])
    for cut in pieces[1:]:
        loudness = loudness * one(*cut)
    return loudness


def centred(rng, extent, scale, reach, split=(), dtype=jnp.bfloat16):
    values = scale * jax.random.normal(rng, extent, jnp.float32)
    if split:
        values = values * block_levels(rng, extent, split, -0.22, 0.18)
    return jnp.clip(values, -reach, reach).astype(dtype)


def setup_inputs(seed: int = 0) -> dict:
    arg_keys = jax.random.split(jax.random.key(seed), 5)
    query = centred(arg_keys[0], (BATCH, HEADS, HEAD_DIM), 2.0, 12.0)
    k_cache = centred(arg_keys[1], (BATCH, SEQ, KV_HEADS, HEAD_DIM), 1.0, 6.0, ((1, 32),))
    v_cache = centred(arg_keys[2], (BATCH, SEQ, KV_HEADS, HEAD_DIM), 1.0, 6.0, ((1, 32),))
    head_gain = jnp.clip(1.0 + 0.1 * jax.random.normal(arg_keys[3], (HEADS, HEAD_DIM), jnp.float32), 0.5, 1.5)
    return dict(query=query, k_cache=k_cache, v_cache=v_cache, head_gain=head_gain)


def reference(query, k_cache, v_cache, head_gain):
    scaling = HEAD_DIM ** (-0.5)

    def per_sequence(inputs):
        query_row, key_rows, value_rows = inputs
        grouped = query_row.astype(jnp.float32).reshape(KV_HEADS, GROUP, HEAD_DIM)
        scores = jnp.einsum('kgd,tkd->kgt', grouped, key_rows.astype(jnp.float32), precision=lax.Precision.HIGHEST) * scaling
        highest = lax.optimization_barrier(jnp.max(scores, axis=-1))
        weights = jnp.exp(scores - highest[..., None])
        total = lax.optimization_barrier(jnp.sum(weights, axis=-1))
        summed = jnp.einsum('kgt,tkd->kgd', weights, value_rows.astype(jnp.float32), precision=lax.Precision.HIGHEST)
        return (highest.reshape(HEADS), total.reshape(HEADS), summed.reshape(HEADS, HEAD_DIM))
    highest, total, summed = lax.map(per_sequence, (query, k_cache, v_cache))
    mixed = summed / total[..., None]
    spread_sq = lax.optimization_barrier(jnp.mean(mixed * mixed, axis=-1, keepdims=True))
    attended = mixed * lax.rsqrt(spread_sq + 1e-06) * head_gain[None, :, :]
    log_norm = highest + jnp.log(total)
    return (attended, log_norm, highest)
```

```python
import functools
import math

import jax
import jax.numpy as jnp
from jax import lax
from jax.experimental import pallas as pl
from jax.experimental.pallas import tpu as pltpu
from jax.sharding import PartitionSpec as P

AXES = ("gx", "gy", "gz")
ROWS = 8
LANES = 128
MESH = pl.DeviceIdType.MESH


def combined_all(part, axis, combine):
    gathered = jax.tree.map(lambda a: lax.all_gather(a, axis), part)

    def take(source):
        return jax.tree.map(lambda a: lax.dynamic_index_in_dim(a, source, 0, False), gathered)

    return lax.fori_loop(
        1, lax.axis_size(axis), lambda source, state: combine(state, take(source)), take(0)
    )


def finish(summed, total, highest, gain_rows):
    mixed = summed / total[..., None]
    spread_sq = jnp.mean(mixed * mixed, axis=-1, keepdims=True)
    return (mixed * lax.rsqrt(spread_sq + 1e-06) * gain_rows, highest + jnp.log(total))


def pair_fold(first_part, second_part):
    peak_one, total_one, summed_one = first_part
    peak_two, total_two, summed_two = second_part
    highest = jnp.maximum(peak_one, peak_two)
    scale_one = jnp.exp(peak_one - highest)
    scale_two = jnp.exp(peak_two - highest)
    total = total_one * scale_one + total_two * scale_two
    summed = summed_one * scale_one[..., None] + summed_two * scale_two[..., None]
    return (highest, total, summed)


def gathered_form(query, k_cache, v_cache, head_gain):
    batch_count, head_count, head_size = query.shape
    kv_count = k_cache.shape[2]
    group_size = head_count // kv_count
    scaling = head_size ** (-0.5)
    grouped = query.reshape(batch_count, kv_count, group_size, head_size)
    scores = (
        jnp.einsum("bkgd,btkd->bkgt", grouped, k_cache, preferred_element_type=jnp.float32)
        * scaling
    )
    local_peak = jnp.max(scores, axis=-1)
    weights = jnp.exp(scores - local_peak[..., None])
    local_total = jnp.sum(weights, axis=-1).reshape(batch_count, head_count)
    local_summed = jnp.einsum(
        "bkgt,btkd->bkgd",
        weights,
        v_cache,
        preferred_element_type=jnp.float32,
        precision=lax.Precision.HIGHEST,
    ).reshape(batch_count, head_count, head_size)
    local_peak = local_peak.reshape(batch_count, head_count)
    partial_value = (local_peak, local_total, local_summed)
    for axis in reversed(AXES):
        partial_value = combined_all(partial_value, axis, pair_fold)
    highest, total, summed = partial_value
    attended, log_norm = finish(summed, total, highest, head_gain[None, :, :])
    return (attended, log_norm, highest)


def local_part(q_rows, keys, values, kv_count, scaling):
    head_count = q_rows.shape[0]
    columns = keys.shape[0]
    group = head_count // kv_count
    raw = lax.dot_general(
        q_rows, keys, (((1,), (1,)), ((), ())), preferred_element_type=jnp.float32
    )
    head_of_row = lax.broadcasted_iota(jnp.int32, (head_count, LANES), 0) // group
    kv_of_lane = lax.broadcasted_iota(jnp.int32, (head_count, LANES), 1) % kv_count
    own = head_of_row == kv_of_lane
    pieces = [
        jnp.where(own, raw[:, c : c + LANES], -jnp.inf) for c in range(0, columns, LANES)
    ]
    peak = jnp.max(functools.reduce(jnp.maximum, pieces), axis=1, keepdims=True)
    factor = scaling * math.log2(math.e)
    high, low, running = [], [], None
    for piece in pieces:
        weight = jnp.exp2((piece - peak) * factor)
        running = weight if running is None else running + weight
        top = weight.astype(jnp.bfloat16)
        high.append(top)
        low.append((weight - top.astype(jnp.float32)).astype(jnp.bfloat16))
    total = jnp.sum(running, axis=1, keepdims=True)
    stacked = jnp.concatenate(
        [jnp.concatenate(high, axis=1), jnp.concatenate(low, axis=1)], axis=0
    )
    both = jnp.dot(stacked, values, preferred_element_type=jnp.float32)
    return peak * scaling, total, both[:head_count] + both[head_count:]


def fused_kernel(
    sizes, batch_count, kv_count, held_back,
    q_ref, k_hbm, v_hbm, gain_ref,
    out_ref, norm_ref, peak_ref,
    k_buf, v_buf, part, part_stat, got, got_stat, fin_stat,
    k_sem, v_sem, send_sem, recv_sem,
):
    size_x, size_y, size_z = sizes
    count = size_x * size_y * size_z
    head_count, head_size = gain_ref.shape
    scaling = head_size ** (-0.5)
    blocks = head_count // ROWS
    me = (lax.axis_index("gx") * size_y + lax.axis_index("gy")) * size_z + lax.axis_index("gz")

    def place(index):
        return (index // (size_y * size_z), (index // size_z) % size_y, index % size_z)

    own_batch = me // blocks
    own_block = me % blocks
    order = [(own_batch + 1 + i) % batch_count for i in range(batch_count)]

    def loads(i):
        return (
            pltpu.make_async_copy(k_hbm.at[order[i]], k_buf.at[i], k_sem.at[i]),
            pltpu.make_async_copy(v_hbm.at[order[i]], v_buf.at[i], v_sem.at[i]),
        )

    for i in range(batch_count):
        for copy in loads(i):
            copy.start()

    barrier = pltpu.get_barrier_semaphore()

    @pl.loop(1, count)
    def _(step):
        pl.semaphore_signal(
            barrier, inc=1, device_id=place((me + step) % count), device_id_type=MESH
        )

    def send_part(owner):
        slot = (me - owner + count) % count
        for which, (src, dst) in enumerate(((part, got), (part_stat, got_stat))):
            pltpu.make_async_remote_copy(
                src_ref=src.at[owner],
                dst_ref=dst.at[slot],
                send_sem=send_sem.at[which],
                recv_sem=recv_sem.at[which],
                device_id=place(owner),
                device_id_type=MESH,
            ).start()

    row = lax.broadcasted_iota(jnp.int32, (ROWS, LANES), 0)
    lane = lax.broadcasted_iota(jnp.int32, (ROWS, LANES), 1)

    def as_lanes(first, second, first_lane, second_lane):
        spread = jnp.where(lane == row + first_lane, first, 0.0) + jnp.where(
            lane == row + second_lane, second, 0.0
        )
        return jnp.sum(spread, axis=0, keepdims=True)

    for i in range(batch_count):
        batch = order[i]
        for copy in loads(i):
            copy.wait()
        peak, total, summed = local_part(
            q_ref[batch], k_buf[i], v_buf[i], kv_count, scaling
        )
        for g in range(blocks):
            rows = slice(g * ROWS, (g + 1) * ROWS)
            part[batch * blocks + g] = summed[rows]
            part_stat[batch * blocks + g] = as_lanes(peak[rows], total[rows], 0, ROWS)
        if i == held_back:
            pl.semaphore_wait(barrier, count - 1)
        if i >= held_back and i < batch_count - 1:
            ready = range(i + 1) if i == held_back else (i,)
            for j in ready:
                for g in range(blocks):
                    send_part(order[j] * blocks + g)
    for step in range(1, blocks):
        send_part(own_batch * blocks + (own_block + step) % blocks)
    got[0] = part[me]
    got_stat[0] = part_stat[me]

    def wait_all(ref, sem):
        span = ref.at[pl.ds(1, count - 1)]
        pltpu.make_async_copy(span, span, sem).wait()

    wait_all(got_stat, recv_sem.at[1])
    stats = got_stat[...].reshape(count, LANES).T
    peaks, totals = stats[:ROWS], stats[ROWS : 2 * ROWS]
    highest = jnp.max(peaks, axis=1, keepdims=True)
    factors = jnp.exp(peaks - highest)
    total = jnp.sum(totals * factors, axis=1, keepdims=True)
    wait_all(got, recv_sem.at[0])
    terms = [got[s] * factors[:, s : s + 1] for s in range(count)]
    while len(terms) > 1:
        terms = [sum(terms[t : t + 2]) for t in range(0, len(terms), 2)]
    gain_rows = gain_ref[pl.ds(pl.multiple_of(own_block * ROWS, ROWS), ROWS), :]
    mixed = terms[0] / total
    spread_sq = jnp.mean(mixed * mixed, axis=1, keepdims=True)
    out_ref[me] = mixed * lax.rsqrt(spread_sq + 1e-06) * gain_rows
    first = own_block * ROWS
    fin_stat[me] = as_lanes(highest + jnp.log(total), highest, first, head_count + first)

    @pl.loop(1, count)
    def _(step):
        peer = place((me + step) % count)
        for which, ref in ((2, out_ref), (3, fin_stat)):
            pltpu.make_async_remote_copy(
                src_ref=ref.at[me],
                dst_ref=ref.at[me],
                send_sem=send_sem.at[which],
                recv_sem=recv_sem.at[which],
                device_id=peer,
                device_id_type=MESH,
            ).start()

    for which, ref in enumerate((part, part_stat, out_ref, fin_stat)):
        wait_all(ref, send_sem.at[which])
    wait_all(fin_stat, recv_sem.at[3])
    for b in range(batch_count):
        line = fin_stat[b * blocks]
        for g in range(1, blocks):
            line = line + fin_stat[b * blocks + g]
        norm_ref[b : b + 1, :] = line[:, :head_count]
        peak_ref[b : b + 1, :] = line[:, head_count : 2 * head_count]
    wait_all(out_ref, recv_sem.at[2])


def fused_form(sizes, query, k_cache, v_cache, head_gain):
    batch_count, head_count, head_size = query.shape
    _, span, kv_count, _ = k_cache.shape
    count = math.prod(sizes)
    columns = span * kv_count
    keys = k_cache.reshape(batch_count, columns, head_size)
    values = v_cache.reshape(batch_count, columns, head_size)
    vmem = pl.BlockSpec(memory_space=pltpu.VMEM)
    hbm = pl.BlockSpec(memory_space=pl.ANY)
    block = (count, ROWS, head_size)
    line = (count, 1, LANES)
    attended, log_norm, highest = pl.pallas_call(
        functools.partial(fused_kernel, sizes, batch_count, kv_count, 3),
        out_shape=(
            jax.ShapeDtypeStruct(block, jnp.float32),
            jax.ShapeDtypeStruct((batch_count, head_count), jnp.float32),
            jax.ShapeDtypeStruct((batch_count, head_count), jnp.float32),
        ),
        in_specs=[vmem, hbm, hbm, vmem],
        out_specs=(vmem, vmem, vmem),
        scratch_shapes=[
            pltpu.VMEM((batch_count, columns, head_size), k_cache.dtype),
            pltpu.VMEM((batch_count, columns, head_size), v_cache.dtype),
            pltpu.VMEM(block, jnp.float32),
            pltpu.VMEM(line, jnp.float32),
            pltpu.VMEM(block, jnp.float32),
            pltpu.VMEM(line, jnp.float32),
            pltpu.VMEM(line, jnp.float32),
            pltpu.SemaphoreType.DMA((batch_count,)),
            pltpu.SemaphoreType.DMA((batch_count,)),
            pltpu.SemaphoreType.DMA((4,)),
            pltpu.SemaphoreType.DMA((4,)),
        ],
        compiler_params=pltpu.CompilerParams(
            collective_id=0, has_side_effects=True, vmem_limit_bytes=48 * 1024 * 1024
        ),
    )(query, keys, values, head_gain)
    return attended.reshape(query.shape), log_norm, highest


def on_device(sizes, query, k_cache, v_cache, head_gain):
    batch_count, head_count, head_size = query.shape
    columns = k_cache.shape[1] * k_cache.shape[2]
    count = math.prod(sizes)
    fits = (
        batch_count * head_count == count * ROWS
        and head_count % ROWS == 0
        and 2 * head_count <= LANES
        and head_size == LANES
        and columns % LANES == 0
        and LANES % k_cache.shape[2] == 0
    )
    if fits:
        return fused_form(sizes, query, k_cache, v_cache, head_gain)
    return gathered_form(query, k_cache, v_cache, head_gain)


def solution(mesh):
    sizes = tuple(mesh.shape[a] for a in AXES)
    in_specs = (P(), P(None, AXES, None, None), P(None, AXES, None, None), P())
    return jax.shard_map(
        functools.partial(on_device, sizes),
        mesh=mesh,
        in_specs=in_specs,
        out_specs=(P(), P(), P()),
        check_vma=False,
    )
```

```python
import functools
import math

import jax
import jax.numpy as jnp
from jax import lax
from jax.experimental import pallas as pl
from jax.experimental.pallas import tpu as pltpu
from jax.sharding import PartitionSpec as P

AXES = ("gx", "gy", "gz")
ROWS = 8
LANES = 128
MESH = pl.DeviceIdType.MESH


def combined_all(part, axis, combine):
    gathered = jax.tree.map(lambda a: lax.all_gather(a, axis), part)

    def take(source):
        return jax.tree.map(lambda a: lax.dynamic_index_in_dim(a, source, 0, False), gathered)

    return lax.fori_loop(
        1, lax.axis_size(axis), lambda source, state: combine(state, take(source)), take(0)
    )


def finish(summed, total, highest, gain_rows):
    mixed = summed / total[..., None]
    spread_sq = jnp.mean(mixed * mixed, axis=-1, keepdims=True)
    return (mixed * lax.rsqrt(spread_sq + 1e-06) * gain_rows, highest + jnp.log(total))


def pair_fold(first_part, second_part):
    peak_one, total_one, summed_one = first_part
    peak_two, total_two, summed_two = second_part
    highest = jnp.maximum(peak_one, peak_two)
    scale_one = jnp.exp(peak_one - highest)
    scale_two = jnp.exp(peak_two - highest)
    total = total_one * scale_one + total_two * scale_two
    summed = summed_one * scale_one[..., None] + summed_two * scale_two[..., None]
    return (highest, total, summed)


def gathered_form(query, k_cache, v_cache, head_gain):
    batch_count, head_count, head_size = query.shape
    kv_count = k_cache.shape[2]
    group_size = head_count // kv_count
    scaling = head_size ** (-0.5)
    grouped = query.reshape(batch_count, kv_count, group_size, head_size)
    scores = (
        jnp.einsum("bkgd,btkd->bkgt", grouped, k_cache, preferred_element_type=jnp.float32)
        * scaling
    )
    local_peak = jnp.max(scores, axis=-1)
    weights = jnp.exp(scores - local_peak[..., None])
    local_total = jnp.sum(weights, axis=-1).reshape(batch_count, head_count)
    local_summed = jnp.einsum(
        "bkgt,btkd->bkgd",
        weights,
        v_cache,
        preferred_element_type=jnp.float32,
        precision=lax.Precision.HIGHEST,
    ).reshape(batch_count, head_count, head_size)
    local_peak = local_peak.reshape(batch_count, head_count)
    partial_value = (local_peak, local_total, local_summed)
    for axis in reversed(AXES):
        partial_value = combined_all(partial_value, axis, pair_fold)
    highest, total, summed = partial_value
    attended, log_norm = finish(summed, total, highest, head_gain[None, :, :])
    return (attended, log_norm, highest)


def local_part(q_rows, keys, values, kv_count, scaling):
    head_count = q_rows.shape[0]
    columns = keys.shape[0]
    group = head_count // kv_count
    raw = lax.dot_general(
        q_rows, keys, (((1,), (1,)), ((), ())), preferred_element_type=jnp.float32
    )
    head_of_row = lax.broadcasted_iota(jnp.int32, (head_count, LANES), 0) // group
    kv_of_lane = lax.broadcasted_iota(jnp.int32, (head_count, LANES), 1) % kv_count
    own = head_of_row == kv_of_lane
    pieces = [
        jnp.where(own, raw[:, c : c + LANES], -jnp.inf) for c in range(0, columns, LANES)
    ]
    peak = jnp.max(functools.reduce(jnp.maximum, pieces), axis=1, keepdims=True)
    factor = scaling * math.log2(math.e)
    high, low, running = [], [], None
    for piece in pieces:
        weight = jnp.exp2((piece - peak) * factor)
        running = weight if running is None else running + weight
        top = weight.astype(jnp.bfloat16)
        high.append(top)
        low.append((weight - top.astype(jnp.float32)).astype(jnp.bfloat16))
    total = jnp.sum(running, axis=1, keepdims=True)
    stacked = jnp.concatenate(
        [jnp.concatenate(high, axis=1), jnp.concatenate(low, axis=1)], axis=0
    )
    both = jnp.dot(stacked, values, preferred_element_type=jnp.float32)
    return peak * scaling, total, both[:head_count] + both[head_count:]


def fused_kernel(
    sizes, batch_count, kv_count, held_back,
    q_hbm, k_hbm, v_hbm, gain_hbm,
    out_ref, norm_ref, peak_ref,
    q_ref, gain_ref, k_buf, v_buf, part, part_stat, got, got_stat, fin_stat,
    side_sem, k_sem, v_sem, send_sem, recv_sem,
):
    size_x, size_y, size_z = sizes
    count = size_x * size_y * size_z
    head_count, head_size = gain_ref.shape
    scaling = head_size ** (-0.5)
    blocks = head_count // ROWS
    me = (lax.axis_index("gx") * size_y + lax.axis_index("gy")) * size_z + lax.axis_index("gz")

    def place(index):
        return (index // (size_y * size_z), (index // size_z) % size_y, index % size_z)

    own_batch = me // blocks
    own_block = me % blocks
    order = [(own_batch + 1 + i) % batch_count for i in range(batch_count)]

    def loads(i):
        return (
            pltpu.make_async_copy(k_hbm.at[order[i]], k_buf.at[i], k_sem.at[i]),
            pltpu.make_async_copy(v_hbm.at[order[i]], v_buf.at[i], v_sem.at[i]),
        )

    q_load = pltpu.make_async_copy(q_hbm, q_ref, side_sem.at[0])
    gain_load = pltpu.make_async_copy(gain_hbm, gain_ref, side_sem.at[1])
    q_load.start()
    for i in range(batch_count):
        for copy in loads(i):
            copy.start()
    gain_load.start()

    barrier = pltpu.get_barrier_semaphore()

    @pl.loop(1, count)
    def _(step):
        pl.semaphore_signal(
            barrier, inc=1, device_id=place((me + step) % count), device_id_type=MESH
        )

    def send_part(owner):
        slot = (me - owner + count) % count
        for which, (src, dst) in enumerate(((part, got), (part_stat, got_stat))):
            pltpu.make_async_remote_copy(
                src_ref=src.at[owner],
                dst_ref=dst.at[slot],
                send_sem=send_sem.at[which],
                recv_sem=recv_sem.at[which],
                device_id=place(owner),
                device_id_type=MESH,
            ).start()

    row = lax.broadcasted_iota(jnp.int32, (ROWS, LANES), 0)
    lane = lax.broadcasted_iota(jnp.int32, (ROWS, LANES), 1)

    def as_lanes(first, second, first_lane, second_lane):
        spread = jnp.where(lane == row + first_lane, first, 0.0) + jnp.where(
            lane == row + second_lane, second, 0.0
        )
        return jnp.sum(spread, axis=0, keepdims=True)

    q_load.wait()
    for i in range(batch_count):
        batch = order[i]
        for copy in loads(i):
            copy.wait()
        peak, total, summed = local_part(
            q_ref[batch], k_buf[i], v_buf[i], kv_count, scaling
        )
        for g in range(blocks):
            rows = slice(g * ROWS, (g + 1) * ROWS)
            part[batch * blocks + g] = summed[rows]
            part_stat[batch * blocks + g] = as_lanes(peak[rows], total[rows], 0, ROWS)
        if i == held_back:
            pl.semaphore_wait(barrier, count - 1)
        if i >= held_back and i < batch_count - 1:
            ready = range(i + 1) if i == held_back else (i,)
            for j in ready:
                for g in range(blocks):
                    send_part(order[j] * blocks + g)
    for step in range(1, blocks):
        send_part(own_batch * blocks + (own_block + step) % blocks)
    got[0] = part[me]
    got_stat[0] = part_stat[me]

    def wait_all(ref, sem):
        span = ref.at[pl.ds(1, count - 1)]
        pltpu.make_async_copy(span, span, sem).wait()

    wait_all(got_stat, recv_sem.at[1])
    stats = got_stat[...].reshape(count, LANES).T
    peaks, totals = stats[:ROWS], stats[ROWS : 2 * ROWS]
    highest = jnp.max(peaks, axis=1, keepdims=True)
    factors = jnp.exp(peaks - highest)
    total = jnp.sum(totals * factors, axis=1, keepdims=True)
    wait_all(got, recv_sem.at[0])
    terms = [got[s] * factors[:, s : s + 1] for s in range(count)]
    while len(terms) > 1:
        terms = [sum(terms[t : t + 2]) for t in range(0, len(terms), 2)]
    gain_load.wait()
    gain_rows = gain_ref[pl.ds(pl.multiple_of(own_block * ROWS, ROWS), ROWS), :]
    mixed = terms[0] / total
    spread_sq = jnp.mean(mixed * mixed, axis=1, keepdims=True)
    out_ref[me] = mixed * lax.rsqrt(spread_sq + 1e-06) * gain_rows
    first = own_block * ROWS
    fin_stat[me] = as_lanes(highest + jnp.log(total), highest, first, head_count + first)

    @pl.loop(1, count)
    def _(step):
        peer = place((me + step) % count)
        for which, ref in ((2, out_ref), (3, fin_stat)):
            pltpu.make_async_remote_copy(
                src_ref=ref.at[me],
                dst_ref=ref.at[me],
                send_sem=send_sem.at[which],
                recv_sem=recv_sem.at[which],
                device_id=peer,
                device_id_type=MESH,
            ).start()

    for which, ref in enumerate((part, part_stat, out_ref, fin_stat)):
        wait_all(ref, send_sem.at[which])
    wait_all(fin_stat, recv_sem.at[3])
    for b in range(batch_count):
        line = fin_stat[b * blocks]
        for g in range(1, blocks):
            line = line + fin_stat[b * blocks + g]
        norm_ref[b : b + 1, :] = line[:, :head_count]
        peak_ref[b : b + 1, :] = line[:, head_count : 2 * head_count]
    wait_all(out_ref, recv_sem.at[2])


def fused_form(sizes, query, k_cache, v_cache, head_gain):
    batch_count, head_count, head_size = query.shape
    _, span, kv_count, _ = k_cache.shape
    count = math.prod(sizes)
    columns = span * kv_count
    keys = k_cache.reshape(batch_count, columns, head_size)
    values = v_cache.reshape(batch_count, columns, head_size)
    vmem = pl.BlockSpec(memory_space=pltpu.VMEM)
    hbm = pl.BlockSpec(memory_space=pltpu.HBM)
    block = (count, ROWS, head_size)
    line = (count, 1, LANES)
    attended, log_norm, highest = pl.pallas_call(
        functools.partial(fused_kernel, sizes, batch_count, kv_count, 3),
        out_shape=(
            jax.ShapeDtypeStruct(block, jnp.float32),
            jax.ShapeDtypeStruct((batch_count, head_count), jnp.float32),
            jax.ShapeDtypeStruct((batch_count, head_count), jnp.float32),
        ),
        in_specs=[hbm] * 4,
        out_specs=(vmem, vmem, vmem),
        scratch_shapes=[
            pltpu.VMEM(query.shape, query.dtype),
            pltpu.VMEM(head_gain.shape, head_gain.dtype),
            pltpu.VMEM((batch_count, columns, head_size), k_cache.dtype),
            pltpu.VMEM((batch_count, columns, head_size), v_cache.dtype),
            pltpu.VMEM(block, jnp.float32),
            pltpu.VMEM(line, jnp.float32),
            pltpu.VMEM(block, jnp.float32),
            pltpu.VMEM(line, jnp.float32),
            pltpu.VMEM(line, jnp.float32),
            pltpu.SemaphoreType.DMA((2,)),
            pltpu.SemaphoreType.DMA((batch_count,)),
            pltpu.SemaphoreType.DMA((batch_count,)),
            pltpu.SemaphoreType.DMA((4,)),
            pltpu.SemaphoreType.DMA((4,)),
        ],
        compiler_params=pltpu.CompilerParams(
            collective_id=0, has_side_effects=True, vmem_limit_bytes=61 * 1024 * 1024
        ),
    )(query, keys, values, head_gain)
    return attended.reshape(query.shape), log_norm, highest


def on_device(sizes, query, k_cache, v_cache, head_gain):
    batch_count, head_count, head_size = query.shape
    columns = k_cache.shape[1] * k_cache.shape[2]
    count = math.prod(sizes)
    fits = (
        batch_count * head_count == count * ROWS
        and head_count % ROWS == 0
        and 2 * head_count <= LANES
        and head_size == LANES
        and columns % LANES == 0
        and LANES % k_cache.shape[2] == 0
    )
    if fits:
        return fused_form(sizes, query, k_cache, v_cache, head_gain)
    return gathered_form(query, k_cache, v_cache, head_gain)


def solution(mesh):
    sizes = tuple(mesh.shape[a] for a in AXES)
    in_specs = (P(), P(None, AXES, None, None), P(None, AXES, None, None), P())
    return jax.shard_map(
        functools.partial(on_device, sizes),
        mesh=mesh,
        in_specs=in_specs,
        out_specs=(P(), P(), P()),
        check_vma=False,
    )
```

```python
import functools
import math

import jax
import jax.numpy as jnp
from jax import lax
from jax.experimental import pallas as pl
from jax.experimental.pallas import tpu as pltpu
from jax.sharding import PartitionSpec as P

AXES = ("gx", "gy", "gz")
ROWS = 8
LANES = 128
MESH = pl.DeviceIdType.MESH


def combined_all(part, axis, combine):
    gathered = jax.tree.map(lambda a: lax.all_gather(a, axis), part)

    def take(source):
        return jax.tree.map(lambda a: lax.dynamic_index_in_dim(a, source, 0, False), gathered)

    return lax.fori_loop(
        1, lax.axis_size(axis), lambda source, state: combine(state, take(source)), take(0)
    )


def finish(summed, total, highest, gain_rows):
    mixed = summed / total[..., None]
    spread_sq = jnp.mean(mixed * mixed, axis=-1, keepdims=True)
    return (mixed * lax.rsqrt(spread_sq + 1e-06) * gain_rows, highest + jnp.log(total))


def pair_fold(first_part, second_part):
    peak_one, total_one, summed_one = first_part
    peak_two, total_two, summed_two = second_part
    highest = jnp.maximum(peak_one, peak_two)
    scale_one = jnp.exp(peak_one - highest)
    scale_two = jnp.exp(peak_two - highest)
    total = total_one * scale_one + total_two * scale_two
    summed = summed_one * scale_one[..., None] + summed_two * scale_two[..., None]
    return (highest, total, summed)


def gathered_form(query, k_cache, v_cache, head_gain):
    batch_count, head_count, head_size = query.shape
    kv_count = k_cache.shape[2]
    group_size = head_count // kv_count
    scaling = head_size ** (-0.5)
    grouped = query.reshape(batch_count, kv_count, group_size, head_size)
    scores = (
        jnp.einsum("bkgd,btkd->bkgt", grouped, k_cache, preferred_element_type=jnp.float32)
        * scaling
    )
    local_peak = jnp.max(scores, axis=-1)
    weights = jnp.exp(scores - local_peak[..., None])
    local_total = jnp.sum(weights, axis=-1).reshape(batch_count, head_count)
    local_summed = jnp.einsum(
        "bkgt,btkd->bkgd",
        weights,
        v_cache,
        preferred_element_type=jnp.float32,
        precision=lax.Precision.HIGHEST,
    ).reshape(batch_count, head_count, head_size)
    local_peak = local_peak.reshape(batch_count, head_count)
    partial_value = (local_peak, local_total, local_summed)
    for axis in reversed(AXES):
        partial_value = combined_all(partial_value, axis, pair_fold)
    highest, total, summed = partial_value
    attended, log_norm = finish(summed, total, highest, head_gain[None, :, :])
    return (attended, log_norm, highest)


def local_part(q_rows, keys, values, kv_count, scaling):
    head_count = q_rows.shape[0]
    columns = keys.shape[0]
    group = head_count // kv_count
    raw = lax.dot_general(
        q_rows, keys, (((1,), (1,)), ((), ())), preferred_element_type=jnp.float32
    )
    head_of_row = lax.broadcasted_iota(jnp.int32, (head_count, LANES), 0) // group
    kv_of_lane = lax.broadcasted_iota(jnp.int32, (head_count, LANES), 1) % kv_count
    own = head_of_row == kv_of_lane
    pieces = [
        jnp.where(own, raw[:, c : c + LANES], -jnp.inf) for c in range(0, columns, LANES)
    ]
    peak = jnp.max(functools.reduce(jnp.maximum, pieces), axis=1, keepdims=True)
    factor = scaling * math.log2(math.e)
    high, low, running = [], [], None
    for piece in pieces:
        weight = jnp.exp2((piece - peak) * factor)
        running = weight if running is None else running + weight
        top = weight.astype(jnp.bfloat16)
        high.append(top)
        low.append((weight - top.astype(jnp.float32)).astype(jnp.bfloat16))
    total = jnp.sum(running, axis=1, keepdims=True)
    stacked = jnp.concatenate(
        [jnp.concatenate(high, axis=1), jnp.concatenate(low, axis=1)], axis=0
    )
    both = jnp.dot(stacked, values, preferred_element_type=jnp.float32)
    return peak * scaling, total, both[:head_count] + both[head_count:]


def fused_kernel(
    sizes, batch_count, kv_count, held_back,
    q_hbm, k_hbm, v_hbm, gain_hbm,
    out_ref, norm_ref, peak_ref,
    q_ref, gain_ref, k_buf, v_buf, part, part_stat, got, got_stat, fin_stat,
    side_sem, k_sem, v_sem, send_sem, recv_sem,
):
    size_x, size_y, size_z = sizes
    count = size_x * size_y * size_z
    head_count, head_size = gain_ref.shape
    scaling = head_size ** (-0.5)
    blocks = head_count // ROWS
    me = (lax.axis_index("gx") * size_y + lax.axis_index("gy")) * size_z + lax.axis_index("gz")

    def place(index):
        return (index // (size_y * size_z), (index // size_z) % size_y, index % size_z)

    own_batch = me // blocks
    own_block = me % blocks
    order = [(own_batch + 1 + i) % batch_count for i in range(batch_count)]

    def loads(i):
        return (
            pltpu.make_async_copy(k_hbm.at[order[i]], k_buf.at[i], k_sem.at[i]),
            pltpu.make_async_copy(v_hbm.at[order[i]], v_buf.at[i], v_sem.at[i]),
        )

    q_load = pltpu.make_async_copy(q_hbm, q_ref, side_sem.at[0])
    gain_load = pltpu.make_async_copy(gain_hbm, gain_ref, side_sem.at[1])
    q_load.start()
    for i in range(batch_count):
        for copy in loads(i):
            copy.start()
    gain_load.start()

    barrier = pltpu.get_barrier_semaphore()

    @pl.loop(1, count)
    def _(step):
        pl.semaphore_signal(
            barrier, inc=1, device_id=place((me + step) % count), device_id_type=MESH
        )

    def send_part(owner):
        slot = (me - owner + count) % count
        for which, (src, dst) in enumerate(((part, got), (part_stat, got_stat))):
            pltpu.make_async_remote_copy(
                src_ref=src.at[owner],
                dst_ref=dst.at[slot],
                send_sem=send_sem.at[which],
                recv_sem=recv_sem.at[which],
                device_id=place(owner),
                device_id_type=MESH,
            ).start()

    row = lax.broadcasted_iota(jnp.int32, (ROWS, LANES), 0)
    lane = lax.broadcasted_iota(jnp.int32, (ROWS, LANES), 1)

    def as_lanes(first, second, first_lane, second_lane):
        spread = jnp.where(lane == row + first_lane, first, 0.0) + jnp.where(
            lane == row + second_lane, second, 0.0
        )
        return jnp.sum(spread, axis=0, keepdims=True)

    q_load.wait()
    for i in range(batch_count):
        batch = order[i]
        for copy in loads(i):
            copy.wait()
        peak, total, summed = local_part(
            q_ref[batch], k_buf[i], v_buf[i], kv_count, scaling
        )
        for g in range(blocks):
            rows = slice(g * ROWS, (g + 1) * ROWS)
            part[batch * blocks + g] = summed[rows]
            part_stat[batch * blocks + g] = as_lanes(peak[rows], total[rows], 0, ROWS)
        if i == held_back:
            pl.semaphore_wait(barrier, count - 1)
        if i >= held_back and i < batch_count - 1:
            ready = range(i + 1) if i == held_back else (i,)
            for j in ready:
                for g in range(blocks):
                    send_part(order[j] * blocks + g)
    for step in range(1, blocks):
        send_part(own_batch * blocks + (own_block + step) % blocks)
    got[0] = part[me]
    got_stat[0] = part_stat[me]

    def wait_all(ref, sem):
        span = ref.at[pl.ds(1, count - 1)]
        pltpu.make_async_copy(span, span, sem).wait()

    wait_all(got_stat, recv_sem.at[1])
    stats = got_stat[...].reshape(count, LANES).T
    peaks, totals = stats[:ROWS], stats[ROWS : 2 * ROWS]
    highest = jnp.max(peaks, axis=1, keepdims=True)
    factors = jnp.exp(peaks - highest)
    total = jnp.sum(totals * factors, axis=1, keepdims=True)
    wait_all(got, recv_sem.at[0])
    terms = [got[s] * factors[:, s : s + 1] for s in range(count)]
    while len(terms) > 1:
        terms = [sum(terms[t : t + 2]) for t in range(0, len(terms), 2)]
    gain_load.wait()
    gain_rows = gain_ref[pl.ds(pl.multiple_of(own_block * ROWS, ROWS), ROWS), :]
    mixed = terms[0] / total
    spread_sq = jnp.mean(mixed * mixed, axis=1, keepdims=True)
    out_ref[me] = mixed * lax.rsqrt(spread_sq + 1e-06) * gain_rows
    first = own_block * ROWS
    fin_stat[me] = as_lanes(highest + jnp.log(total), highest, first, head_count + first)

    @pl.loop(1, count)
    def _(step):
        peer = place((me + step) % count)
        for which, ref in ((2, out_ref), (3, fin_stat)):
            pltpu.make_async_remote_copy(
                src_ref=ref.at[me],
                dst_ref=ref.at[me],
                send_sem=send_sem.at[which],
                recv_sem=recv_sem.at[which],
                device_id=peer,
                device_id_type=MESH,
            ).start()

    for which, ref in enumerate((part, part_stat, out_ref, fin_stat)):
        wait_all(ref, send_sem.at[which])
    wait_all(fin_stat, recv_sem.at[3])
    for b in range(batch_count):
        line = fin_stat[b * blocks]
        for g in range(1, blocks):
            line = line + fin_stat[b * blocks + g]
        norm_ref[b : b + 1, :] = line[:, :head_count]
        peak_ref[b : b + 1, :] = line[:, head_count : 2 * head_count]
    wait_all(out_ref, recv_sem.at[2])


def fused_form(sizes, query, k_cache, v_cache, head_gain):
    batch_count, head_count, head_size = query.shape
    _, span, kv_count, _ = k_cache.shape
    count = math.prod(sizes)
    columns = span * kv_count
    keys = k_cache.reshape(batch_count, columns, head_size)
    values = v_cache.reshape(batch_count, columns, head_size)
    vmem = pl.BlockSpec(memory_space=pltpu.VMEM)
    hbm = pl.BlockSpec(memory_space=pltpu.HBM)
    block = (count, ROWS, head_size)
    line = (count, 1, LANES)
    attended, log_norm, highest = pl.pallas_call(
        functools.partial(fused_kernel, sizes, batch_count, kv_count, 3),
        out_shape=(
            jax.ShapeDtypeStruct(block, jnp.float32),
            jax.ShapeDtypeStruct((batch_count, head_count), jnp.float32),
            jax.ShapeDtypeStruct((batch_count, head_count), jnp.float32),
        ),
        in_specs=[hbm] * 4,
        out_specs=(vmem, vmem, vmem),
        scratch_shapes=[
            pltpu.VMEM(query.shape, query.dtype),
            pltpu.VMEM(head_gain.shape, head_gain.dtype),
            pltpu.VMEM((batch_count, columns, head_size), k_cache.dtype),
            pltpu.VMEM((batch_count, columns, head_size), v_cache.dtype),
            pltpu.VMEM(block, jnp.float32),
            pltpu.VMEM(line, jnp.float32),
            pltpu.VMEM(block, jnp.float32),
            pltpu.VMEM(line, jnp.float32),
            pltpu.VMEM(line, jnp.float32),
            pltpu.SemaphoreType.DMA((2,)),
            pltpu.SemaphoreType.DMA((batch_count,)),
            pltpu.SemaphoreType.DMA((batch_count,)),
            pltpu.SemaphoreType.DMA((4,)),
            pltpu.SemaphoreType.DMA((4,)),
        ],
        compiler_params=pltpu.CompilerParams(
            collective_id=0, has_side_effects=True, vmem_limit_bytes=48 * 1024 * 1024
        ),
    )(*(pltpu.with_memory_space_constraint(a, pltpu.HBM) for a in (query, keys, values, head_gain)))
    return attended.reshape(query.shape), log_norm, highest


def on_device(sizes, query, k_cache, v_cache, head_gain):
    batch_count, head_count, head_size = query.shape
    columns = k_cache.shape[1] * k_cache.shape[2]
    count = math.prod(sizes)
    fits = (
        batch_count * head_count == count * ROWS
        and head_count % ROWS == 0
        and 2 * head_count <= LANES
        and head_size == LANES
        and columns % LANES == 0
        and LANES % k_cache.shape[2] == 0
    )
    if fits:
        return fused_form(sizes, query, k_cache, v_cache, head_gain)
    return gathered_form(query, k_cache, v_cache, head_gain)


def solution(mesh):
    sizes = tuple(mesh.shape[a] for a in AXES)
    in_specs = (P(), P(None, AXES, None, None), P(None, AXES, None, None), P())
    return jax.shard_map(
        functools.partial(on_device, sizes),
        mesh=mesh,
        in_specs=in_specs,
        out_specs=(P(), P(), P()),
        check_vma=False,
    )
```
